1024 devices in a mesh: gx: 8 (over z), gy: 8 (over x), gz: 16 (over y, core).
Axes of the slice: x: 8, y: 8, z: 8, core: 2. Of those that a mesh axis runs over, the one named last changes fastest.
Arguments:
- fine_rhs: float32 [3072, 32, 1024], P(('gx', 'gy', 'gz')), may hold values from -6 to 6
- coarse_rhs: float32 [256, 256, 2048], P('gx', 'gy', 'gz'), may hold values from -6 to 6
- patch_count: int32 [1024], P(('gx', 'gy', 'gz')), may hold values from 2 to 3, as said below
- patch_corner: int32 [3072, 3], P(('gx', 'gy', 'gz')), may hold values from 0 to 2032, as said below
Outputs:
- fine_solution: float32 [3072, 32, 1024], P(('gx', 'gy', 'gz'))
- coarse_solution: float32 [256, 256, 2048], P('gx', 'gy', 'gz')
The draws below stay inside these ranges and needn't reach their ends.
Inputs may be any that keep to these rules, and one draw needn't show every extreme that they name: Slots 0 to patch_count[d] - 1 of device d hold live patches, the others are unused. `patch_corner`: A live patch's footprint starts at a multiple of 16 in each dimension and lies inside the coarse block of one device with the same gx and gy indices as the patch's owner; live footprints never intersect; at most 2 live patches of one device lie in the block of any one device. Rows of unused slots are zero.
All inputs are finite; a program needn't handle non-finite values.
Results may differ from the reference program's by a relative error of at most 0.00007.
Values sent between devices are 32-bit elements; how exact they have to be, the bound alone decides.
A program may use at most 64 MiB of HBM per device.

```python
import jax
import jax.numpy as jnp
from jax import lax

PATCH = 32
FOOT = 16
SLOTS = 3
CAP = 2
CX = 32
CY = 32
CZ = 128
SWEEPS = 3
FINE_SWEEPS = 2
NX = 256
NY = 256
NZ = 2048
PATCHES = 3072
N_GX = 8
N_GY = 8
N_GZ = 16


def patch_layout(key):
    base_key = jax.random.fold_in(key, 4242)
    key_hot, key_count, key_busy, key_order, key_place = jax.random.split(base_key, 5)
    columns = N_GX * N_GY
    group_size = N_GZ
    spots_first = CX // FOOT
    spots_second = CY // FOOT
    spots_third = CZ // FOOT
    spot_total = spots_first * spots_second * spots_third
    hottest = jax.random.randint(key_hot, (columns,), 0, group_size)
    counts = jax.random.randint(key_count, (columns, group_size), CAP, max(SLOTS // 2, CAP) + 1)
    busiest = jax.random.randint(key_busy, (columns,), 0, group_size)
    owners = jnp.arange(group_size, dtype=jnp.int32)
    counts = jnp.where(owners[None, :] == busiest[:, None], SLOTS, counts)
    scores = jax.random.randint(key_order, (columns, group_size, group_size), 0, 1 << 20) * group_size + owners[None, None, :]
    scores = jnp.where(owners[None, None, :] == hottest[:, None, None], -1, scores)
    home_order = jnp.argsort(scores, axis=2)
    slot_range = jnp.arange(SLOTS, dtype=jnp.int32)
    home_slot = home_order[:, :, slot_range // CAP]
    spot_range = jnp.arange(spot_total, dtype=jnp.int32)
    spot_scores = jax.random.randint(key_place, (columns, group_size, spot_total), 0, 1 << 20) * spot_total + spot_range[None, None, :]
    places = jnp.argsort(spot_scores, axis=2)
    pick_rank = owners[None, :, None] * CAP + (slot_range % CAP)[None, None, :]
    pick_rank = jnp.broadcast_to(pick_rank, (columns, group_size, SLOTS))
    column_index = jnp.broadcast_to(jnp.arange(columns, dtype=jnp.int32)[:, None, None], (columns, group_size, SLOTS))
    spot_index = places[column_index, home_slot, pick_rank]
    spot_first = spot_index // (spots_second * spots_third)
    spot_second = spot_index // spots_third % spots_second
    spot_third = spot_index % spots_third
    column_range = jnp.arange(columns, dtype=jnp.int32)
    base_first = column_range // N_GY * CX
    base_second = column_range % N_GY * CY
    corner_first = base_first[:, None, None] + spot_first * FOOT
    corner_second = base_second[:, None, None] + spot_second * FOOT
    corner_third = home_slot * CZ + spot_third * FOOT
    alive_mask = slot_range[None, None, :] < counts[:, :, None]
    corners = jnp.stack([corner_first, corner_second, corner_third], -1) * alive_mask[:, :, :, None].astype(jnp.int32)
    return (counts.reshape(-1).astype(jnp.int32), corners.reshape(-1, 3).astype(jnp.int32))


def draw_patch_count(key, part):
    return patch_layout(key)[0]


def draw_patch_corner(key, part):
    return patch_layout(key)[1]


def draw_coarse_rhs(key, part):
    key_noise = jax.random.fold_in(key, 17)
    return jnp.clip(jax.random.normal(key_noise, (NX, NY, NZ), jnp.float32), -6.0, 6.0)


def steps_of(rng, dims, pieces, least, high):
    level, own = 1.0, jax.random.fold_in(rng, 6)
    for dim, parts in pieces:
        draws = jnp.exp(jax.random.uniform(jax.random.fold_in(own, dim), (parts,), jnp.float32, least / len(pieces), high / len(pieces)))
        level = level * jnp.repeat(draws, dims[dim] // parts).reshape([-1 if axis == dim else 1 for axis in range(len(dims))])
    return level


def bell_draw(rng, extent, width, bound, cuts=(), held_as=jnp.bfloat16):
    level = steps_of(rng, extent, cuts, -0.22, 0.18) if cuts else 1.0
    entries = jax.random.normal(rng, extent, jnp.float32) * width * level
    return jnp.minimum(jnp.maximum(entries, -bound), bound).astype(held_as)


def setup_inputs(seed: int = 0) -> dict:
    streams_of = jax.random.split(jax.random.key(seed), 5)
    fine_rhs = bell_draw(streams_of[0], (PATCHES, PATCH, PATCH * PATCH), 1.0, 6.0, ((0, 1024),), jnp.float32)
    coarse_rhs = draw_coarse_rhs(jax.random.fold_in(streams_of[4], 71), 0)
    patch_count = draw_patch_count(jax.random.fold_in(streams_of[4], 71), 0)
    patch_corner = draw_patch_corner(jax.random.fold_in(streams_of[4], 71), 0)
    return {"fine_rhs": fine_rhs, "coarse_rhs": coarse_rhs, "patch_count": patch_count, "patch_corner": patch_corner}


RELAX_WEIGHT = 0.9


def neighbors(padded):
    total = padded[2:, 1:-1, 1:-1] + padded[:-2, 1:-1, 1:-1]
    total = total + padded[1:-1, 2:, 1:-1] + padded[1:-1, :-2, 1:-1]
    return total + padded[1:-1, 1:-1, 2:] + padded[1:-1, 1:-1, :-2]


def relax_step(values_now, right_side, rim_values):
    total = neighbors(jnp.pad(values_now, 1) + rim_values)
    return values_now + RELAX_WEIGHT * (right_side - (6.0 * values_now - total)) / 6.0


def broaden(face_rows):
    return jnp.repeat(jnp.repeat(face_rows, 2, 0), 2, 1)


def pre_patch(right_side):
    rim_values = jnp.zeros_like(jnp.pad(right_side, 1))
    values_now = jnp.zeros_like(right_side)
    for iteration in range(FINE_SWEEPS):
        values_now = relax_step(values_now, right_side, rim_values)
    residual = right_side - (6.0 * values_now - neighbors(jnp.pad(values_now, 1)))
    averages = 0.5 * residual.reshape(FOOT, 2, FOOT, 2, FOOT, 2).sum(axis=(1, 3, 5))
    return values_now, averages


def post_patch(right_side, start_values, coarse_cube):
    parent = coarse_cube[1:-1, 1:-1, 1:-1]
    lifted = jnp.repeat(jnp.repeat(jnp.repeat(parent, 2, 0), 2, 1), 2, 2)
    rim_values = jnp.zeros_like(jnp.pad(right_side, 1))
    rim_values = rim_values.at[0, 1:-1, 1:-1].set(broaden(coarse_cube[0, 1:-1, 1:-1]))
    rim_values = rim_values.at[-1, 1:-1, 1:-1].set(broaden(coarse_cube[-1, 1:-1, 1:-1]))
    rim_values = rim_values.at[1:-1, 0, 1:-1].set(broaden(coarse_cube[1:-1, 0, 1:-1]))
    rim_values = rim_values.at[1:-1, -1, 1:-1].set(broaden(coarse_cube[1:-1, -1, 1:-1]))
    rim_values = rim_values.at[1:-1, 1:-1, 0].set(broaden(coarse_cube[1:-1, 1:-1, 0]))
    rim_values = rim_values.at[1:-1, 1:-1, -1].set(broaden(coarse_cube[1:-1, 1:-1, -1]))
    values_now = start_values + lifted
    for iteration in range(FINE_SWEEPS):
        values_now = relax_step(values_now, right_side, rim_values)
    return values_now


def reference(fine_rhs, coarse_rhs, patch_count, patch_corner):
    patch_total = fine_rhs.shape[0]
    owners = patch_total // SLOTS
    cubes_in = fine_rhs.reshape(owners, SLOTS, PATCH, PATCH, PATCH)
    fine_pre, averages = lax.map(jax.vmap(pre_patch), cubes_in)
    patch_range = jnp.arange(patch_total, dtype=jnp.int32)
    alive_mask = (patch_range % SLOTS) < patch_count[patch_range // SLOTS]
    cells_first, cells_second, cells_third = coarse_rhs.shape
    spots_first = cells_first // FOOT
    spots_second = cells_second // FOOT
    spots_third = cells_third // FOOT
    spot_coords = patch_corner // FOOT
    spot_first = jnp.where(alive_mask, spot_coords[:, 0], spots_first).astype(jnp.int32)
    spot_second = jnp.where(alive_mask, spot_coords[:, 1], spots_second).astype(jnp.int32)
    spot_third = jnp.where(alive_mask, spot_coords[:, 2], spots_third).astype(jnp.int32)
    placed = jnp.zeros((spots_first, spots_second, spots_third, FOOT, FOOT, FOOT), jnp.float32)
    placed = placed.at[spot_first, spot_second, spot_third].set(averages.reshape(patch_total, FOOT, FOOT, FOOT), mode="drop")
    covered = jnp.zeros((spots_first, spots_second, spots_third), jnp.float32)
    covered = covered.at[spot_first, spot_second, spot_third].set(1.0, mode="drop")
    blocks = coarse_rhs.reshape(spots_first, FOOT, spots_second, FOOT, spots_third, FOOT).transpose(0, 2, 4, 1, 3, 5)
    blocks = jnp.where(covered[:, :, :, None, None, None] > 0.5, placed, blocks)
    composite = blocks.transpose(0, 3, 1, 4, 2, 5).reshape(cells_first, cells_second, cells_third)
    solution = RELAX_WEIGHT * composite / 6.0
    for iteration in range(SWEEPS - 1):
        solution = solution + RELAX_WEIGHT * (composite - (6.0 * solution - neighbors(jnp.pad(solution, 1)))) / 6.0
    padded = jnp.pad(solution, 1)

    def cut_cube(corner_row):
        return lax.dynamic_slice(padded, (corner_row[0], corner_row[1], corner_row[2]), (FOOT + 2, FOOT + 2, FOOT + 2))

    def finish_patches(packed):
        right_rows, start_rows, corner_rows, alive_rows = packed
        coarse_cubes = jax.vmap(cut_cube)(corner_rows)
        results = jax.vmap(post_patch)(right_rows, start_rows, coarse_cubes)
        return results * alive_rows.astype(jnp.float32)[:, None, None, None]

    finished = lax.map(finish_patches, (cubes_in, fine_pre, patch_corner.reshape(owners, SLOTS, 3), alive_mask.reshape(owners, SLOTS)))
    return finished.reshape(fine_rhs.shape), solution
```

```python
import functools

import jax
import jax.numpy as jnp
from jax import lax
from jax.experimental import pallas as pl
from jax.experimental.pallas import tpu as pltpu
from jax.sharding import PartitionSpec as P

MESH = pl.DeviceIdType.MESH
SLOTS = 3
EDGE = 32
FOOT = 16
LANES = 128
SPOTS = 32
REC = 24


def iota(shape, dim):
    return lax.broadcasted_iota(jnp.int32, shape, dim)


def rolled(values, shift, axis):
    shift = shift % values.shape[axis]
    return values if shift == 0 else pltpu.roll(values, shift, axis)


def fine_sum(v):
    row = iota(v.shape, 0) % EDGE
    lane = iota(v.shape, 1)
    z = lane % EDGE
    total = jnp.where(row > 0, rolled(v, 1, 0), 0.0) + jnp.where(row < EDGE - 1, rolled(v, -1, 0), 0.0)
    total += jnp.where(lane >= EDGE, rolled(v, EDGE, 1), 0.0)
    total += jnp.where(lane < EDGE * (EDGE - 1), rolled(v, -EDGE, 1), 0.0)
    total += jnp.where(z > 0, rolled(v, 1, 1), 0.0)
    return total + jnp.where(z < EDGE - 1, rolled(v, -1, 1), 0.0)


def split3(v):
    high = v.astype(jnp.bfloat16)
    rest = v - high.astype(jnp.float32)
    middle = rest.astype(jnp.bfloat16)
    low = (rest - middle.astype(jnp.float32)).astype(jnp.bfloat16)
    return high, middle, low


def select_dot(v, chosen, dims):
    total = None
    for part in reversed(split3(v)):
        term = lax.dot_general(part, chosen, (dims, ((), ())), preferred_element_type=jnp.float32)
        total = term if total is None else total + term
    return total


def expand_matrix():
    lane = iota((1, EDGE * EDGE), 1)
    key = (lane // (2 * EDGE)) * FOOT + (lane % EDGE) // 2
    row = iota((FOOT * FOOT, EDGE * EDGE), 0)
    return jnp.where(row == key, 1.0, 0.0).astype(jnp.bfloat16)


def face_matrix():
    lane = iota((1, EDGE * EDGE), 1)
    y, z = lane // EDGE, lane % EDGE
    row = iota((LANES, EDGE * EDGE), 0) % 64
    hit = row == jnp.where(y == 0, z // 2, -1)
    hit |= row == jnp.where(y == EDGE - 1, FOOT + z // 2, -1)
    hit |= row == jnp.where(z == 0, 2 * FOOT + y // 2, -1)
    hit |= row == jnp.where(z == EDGE - 1, 3 * FOOT + y // 2, -1)
    return jnp.where(hit, 1.0, 0.0).astype(jnp.bfloat16)


def pre_kernel(count_ref, corner_ref, fine_ref, averages_ref, codes_ref, sums):
    row = iota((8, LANES), 0)
    codes = jnp.full((8, LANES), -1, jnp.int32)
    for slot in range(SLOTS):
        first, second, third = (corner_ref[slot, dim] for dim in range(3))
        spot = lax.div(lax.rem(first, EDGE), FOOT) * 2 + lax.div(lax.rem(second, EDGE), FOOT)
        spot = spot * 8 + lax.div(lax.rem(third, LANES), FOOT)
        code = jnp.where(slot < count_ref[0], lax.div(third, LANES) * SPOTS + spot, -1)
        codes = jnp.where(row == slot, code, codes)
    codes_ref[...] = codes
    right = fine_ref[...]
    pre = 0.165 * right + 0.0225 * fine_sum(right)
    residual = right - 6.0 * pre + fine_sum(pre)
    coarse = select_dot(residual, expand_matrix(), ((1,), (1,)))
    rows = SLOTS * FOOT
    for part in range(2):
        lanes = slice(part * LANES, (part + 1) * LANES)
        sums[part] = coarse[:, lanes]
        averages_ref[:, lanes] = 0.5 * (
            sums[part, pl.ds(0, rows, stride=2), :] + sums[part, pl.ds(1, rows, stride=2), :]
        )


def post_kernel(count_ref, fine_ref, record_ref, out_ref, parent, faces):
    right = fine_ref[...]
    pre = 0.165 * right + 0.0225 * fine_sum(right)
    lane = iota((FOOT, LANES), 1)
    low_rows, high_rows = [], []
    for slot in range(SLOTS):
        first = slot * REC
        for odd in range(2):
            for part in range(2):
                parent[part, pl.ds(slot * EDGE + odd, FOOT, stride=2), :] = record_ref[
                    pl.ds(first, FOOT), part * LANES : (part + 1) * LANES
                ]
        tile = record_ref[pl.ds(first + FOOT, 8), 0:LANES]
        for odd in range(2):
            faces[pl.ds(slot * EDGE + odd, 8, stride=2), :] = tile
            faces[pl.ds(slot * EDGE + FOOT + odd, 8, stride=2), :] = tile
        side = record_ref[pl.ds(first + FOOT, 8), LANES : 2 * LANES]
        low_rows.append(jnp.concatenate([side[0:1], side[1:2]], 1))
        high_rows.append(jnp.concatenate([side[2:3], side[3:4]], 1))
    expand = expand_matrix()
    lifted = select_dot(jnp.concatenate([parent[0], parent[1]], 1), expand, ((1,), (0,)))
    row = iota((SLOTS * EDGE, LANES), 0) % EDGE
    wanted = (row >= FOOT) == (iota((SLOTS * EDGE, LANES), 1) >= 64)
    ghost = select_dot(jnp.where(wanted, faces[...], 0.0), face_matrix(), ((1,), (0,)))
    spare = jnp.zeros((2, FOOT * FOOT), jnp.float32)
    ends = select_dot(jnp.concatenate(low_rows + high_rows + [spare], 0), expand, ((1,), (0,)))
    value = pre + lifted
    row = iota((EDGE, EDGE * EDGE), 0)
    count = count_ref[0]
    for slot in range(SLOTS):
        rows = slice(slot * EDGE, (slot + 1) * EDGE)
        now = value[rows]
        fixed = right[rows] + ghost[rows]
        fixed += jnp.where(row == 0, ends[slot : slot + 1], 0.0)
        fixed += jnp.where(row == EDGE - 1, ends[SLOTS + slot : SLOTS + slot + 1], 0.0)
        for _ in range(2):
            now = 0.1 * now + 0.15 * (fixed + fine_sum(now))
        out_ref[rows, :] = jnp.where(slot < count, now, 0.0)


def coarse_kernel(
    sizes,
    codes_ref,
    averages_ref,
    coarse_ref,
    solution_ref,
    record_ref,
    gathered,
    meta,
    table,
    table_smem,
    level1,
    level2,
    level3,
    x_out,
    x_in,
    z_out,
    z_in,
    records,
    pre_out,
    pre_in,
    chain_out,
    chain_in,
    ring_send,
    ring_recv,
    pair_send,
    pair_recv,
    halo_send,
    halo_recv,
    pre_send,
    pre_recv,
    chain_send,
    chain_recv,
    table_sem,
):
    n_x, n_y, n_z = sizes
    chips = n_z // 2
    half = chips // 2
    gx, gy, me = lax.axis_index("gx"), lax.axis_index("gy"), lax.axis_index("gz")
    chip, core = lax.div(me, 2), lax.rem(me, 2)
    sign = 1 - 2 * core
    pair = me + sign
    ring = tuple(lax.rem(chip + step * sign + chips, chips) * 2 + core for step in (1, -1))
    z_near = tuple(lax.rem(me + step + n_z, n_z) for step in (-1, 1))
    y_near = tuple(lax.rem(gy + step + n_y, n_y) for step in (-1, 1))
    x_near = tuple(lax.rem(gx + step + n_x, n_x) for step in (-1, 1))
    lane = iota((FOOT, LANES), 1)
    group = lane // FOOT

    barrier = pltpu.get_barrier_semaphore()
    greeted = [{"gz": d} for d in ring + z_near] + [{"gy": d} for d in y_near] + [{"gx": d} for d in x_near]
    for device in greeted:
        pl.semaphore_signal(barrier, inc=1, device_id=device, device_id_type=MESH)

    row8 = iota((8, LANES), 0)
    meta[me] = codes_ref[...]
    for slot in range(SLOTS):
        gathered[me * SLOTS + slot] = averages_ref[pl.ds(slot * FOOT, FOOT), :]
    pl.semaphore_wait(barrier, len(greeted))

    def send(source, target, send_sem, recv_sem, device):
        copy = pltpu.make_async_remote_copy(
            src_ref=source,
            dst_ref=target,
            send_sem=send_sem,
            recv_sem=recv_sem,
            device_id=device,
            device_id_type=MESH,
        )
        copy.start()
        return copy

    started = []

    items = (SLOTS,) + tuple(range(SLOTS))
    takes = ((SLOTS, 0, 1), (2,))

    def carried(way, hop, item):
        return hop < half or item in takes[way]

    def place(owner, item):
        return meta.at[owner] if item == SLOTS else gathered.at[owner * SLOTS + item]

    def owner_of(way, hop):
        step = hop if way == 0 else -hop
        return lax.rem(chip - step * sign + chips, chips) * 2 + core

    ring_copies, pair_copies = {}, []
    for item in items:
        for way in range(2):
            if carried(way, 1, item):
                ring_copies[way, 1, item] = send(
                    place(me, item),
                    place(me, item),
                    ring_send.at[way, 0, item],
                    ring_recv.at[way, 0, item],
                    {"gz": ring[way]},
                )
        pair_copies.append(
            send(place(me, item), place(me, item), pair_send.at[0, 0, item], pair_recv.at[0, 0, item], {"gz": pair})
        )
    for hop in range(1, half + 1):
        for item in items:
            for way in range(2):
                if not carried(way, hop, item):
                    continue
                ring_copies[way, hop, item].wait_recv()
                here = place(owner_of(way, hop), item)
                if hop < half and carried(way, hop + 1, item):
                    ring_copies[way, hop + 1, item] = send(
                        here,
                        here,
                        ring_send.at[way, hop, item],
                        ring_recv.at[way, hop, item],
                        {"gz": ring[way]},
                    )
                pair_copies.append(
                    send(here, here, pair_send.at[way, hop, item], pair_recv.at[way, hop, item], {"gz": pair})
                )
    started += list(ring_copies.values()) + pair_copies
    for number, copy in enumerate(pair_copies):
        copy.wait_recv()

    lane8 = iota((8, LANES), 1)
    sources = jnp.zeros((8, LANES), jnp.int32)
    spots = jnp.full((8, LANES), SPOTS, jnp.int32)
    for owner in range(n_z):
        codes = meta[owner] - me * SPOTS
        live = (codes >= 0) & (codes < SPOTS) & (row8 < SLOTS)
        hit = live & (codes == lane8)
        sources = jnp.maximum(sources, jnp.where(hit, owner * SLOTS + row8 + 1, 0))
        spots = jnp.where((lane8 == owner) & live, codes, spots)
    source = jnp.maximum(jnp.maximum(sources[0:1], sources[1:2]), sources[2:3])
    source = jnp.broadcast_to(source, (8, LANES))
    covers = jnp.where(source > 0, lane8 % 8, -1)
    table[pl.ds(0, 8), :] = jnp.where(row8 == 0, jnp.maximum(source - 1, 0), covers)
    table[pl.ds(8, 8), :] = spots
    table_copy = pltpu.make_async_copy(table, table_smem, table_sem)
    table_copy.start()
    table_copy.wait()

    for sx in range(2):
        for sy in range(2):
            cubes, masks = [], []
            for sz in range(8):
                spot = (sx * 2 + sy) * 8 + sz
                cubes.append(gathered[table_smem[0, spot]])
                masks.append(group == table_smem[1, spot])
            for second in range(FOOT):
                part, place_in = second // 8, second % 8
                y = sy * FOOT + second
                plane = coarse_ref[pl.ds(sx * FOOT * EDGE + y, FOOT, stride=EDGE), :]
                for sz in range(8):
                    cube = cubes[sz][:, part * LANES : (part + 1) * LANES]
                    plane = jnp.where(masks[sz], rolled(cube, FOOT * (sz - place_in), 1), plane)
                level1[pl.ds((y + 1) * EDGE + sx * FOOT, FOOT), :] = plane

    lane32 = iota((EDGE, LANES), 1)
    row32 = iota((EDGE, LANES), 0)

    def start_halo(number, level):
        x_out[number, 0] = level[pl.ds(EDGE, EDGE, stride=EDGE), :]
        x_out[number, 1] = level[pl.ds(EDGE + EDGE - 1, EDGE, stride=EDGE), :]
        low = jnp.zeros((EDGE, LANES), jnp.float32)
        high = jnp.zeros((EDGE, LANES), jnp.float32)
        for y in range(EDGE):
            plane = level[pl.ds((y + 1) * EDGE, EDGE), :]
            low = jnp.where(lane32 == y, rolled(plane, y, 1), low)
            high = jnp.where(lane32 == y, rolled(plane, y - (LANES - 1), 1), high)
        z_out[number, 0] = low
        z_out[number, 1] = high
        copies = []
        for side in range(2):
            other = 1 - side
            copies.append(
                send(
                    x_out.at[number, side],
                    x_in.at[number, other],
                    halo_send.at[number, side],
                    halo_recv.at[number, other],
                    {"gx": x_near[side]},
                )
            )
            copies.append(
                send(
                    level.at[pl.ds(EDGE if side == 0 else EDGE * EDGE, EDGE)],
                    level.at[pl.ds((EDGE + 1) * EDGE if side == 0 else 0, EDGE)],
                    halo_send.at[number, 2 + side],
                    halo_recv.at[number, 2 + other],
                    {"gy": y_near[side]},
                )
            )
            copies.append(
                send(
                    z_out.at[number, side],
                    z_in.at[number, other],
                    halo_send.at[number, 4 + side],
                    halo_recv.at[number, 4 + other],
                    {"gz": z_near[side]},
                )
            )
        return copies

    def finish_halo(number, level, copies):
        for copy in copies:
            copy.wait_recv()
        started.extend(copies)
        for side in range(2):
            inside = (gx > 0, gy > 0, me > 0) if side == 0 else (gx < n_x - 1, gy < n_y - 1, me < n_z - 1)
            x_in[number, side] = jnp.where(inside[0], x_in[number, side], 0.0)
            edge = pl.ds(0 if side == 0 else (EDGE + 1) * EDGE, EDGE)
            level[edge, :] = jnp.where(inside[1], level[edge, :], 0.0)
            z_in[number, side] = jnp.where(inside[2], z_in[number, side], 0.0)

    def sweep(number, level, out, weights):
        z_low, z_high = z_in[number, 0], z_in[number, 1]
        for y in range(EDGE):
            plane = level[pl.ds((y + 1) * EDGE, EDGE), :]
            total = level[pl.ds(y * EDGE, EDGE), :] + level[pl.ds((y + 2) * EDGE, EDGE), :]
            x_low, x_high = x_in[number, 0, pl.ds(y, 1), :], x_in[number, 1, pl.ds(y, 1), :]
            total += jnp.where(row32 == 0, x_low, rolled(plane, 1, 0))
            total += jnp.where(row32 == EDGE - 1, x_high, rolled(plane, -1, 0))
            total += jnp.where(lane32 == 0, rolled(z_low, -y, 1), rolled(plane, 1, 1))
            total += jnp.where(
                lane32 == LANES - 1, rolled(z_high, LANES - 1 - y, 1), rolled(plane, -1, 1)
            )
            if weights is None:
                value = 0.165 * plane + 0.0225 * total
            else:
                value = 0.1 * plane + 0.15 * (level1[pl.ds((y + 1) * EDGE, EDGE), :] + total)
            out[pl.ds((y + 1) * EDGE, EDGE), :] = value
            if weights is not None:
                solution_ref[pl.ds(y, EDGE, stride=EDGE), :] = value

    copies = start_halo(0, level1)
    finish_halo(0, level1, copies)
    sweep(0, level1, level2, None)
    copies = start_halo(1, level2)
    finish_halo(1, level2, copies)
    sweep(1, level2, level3, 1)
    copies = start_halo(2, level3)
    finish_halo(2, level3, copies)

    for sx in range(2):
        rows = pl.ds(sx * FOOT, FOOT)
        for sy in range(2):
            planes = [
                level3[pl.ds((sy * FOOT + second) * EDGE + sx * FOOT, FOOT), :] for second in range(FOOT + 2)
            ]
            upper = jnp.zeros((FOOT, LANES), jnp.float32)
            lower = jnp.zeros((FOOT, LANES), jnp.float32)
            for second in range(FOOT):
                here = lane % FOOT == second
                upper = jnp.where(here, rolled(planes[second + 1], second - (FOOT - 1), 1), upper)
                lower = jnp.where(here, rolled(planes[second + 1], second, 1), lower)
            ends = []
            for side in range(2):
                if side == sx:
                    face = x_in[2, side, pl.ds(sy * FOOT, FOOT), :]
                else:
                    x = FOOT - 1 if side == 0 else FOOT
                    face = level3[pl.ds((sy * FOOT + 1) * EDGE + x, FOOT, stride=EDGE), :]
                for part in range(2):
                    tile = face[part * 8 : part * 8 + 8]
                    turned = jnp.zeros((8, LANES), jnp.float32)
                    for step in range(8):
                        moved = rolled(rolled(tile, -step, 0), FOOT * step, 1)
                        turned = jnp.where((lane8 // FOOT - row8 + 8) % 8 == step, moved, turned)
                    ends.append(turned)
            for sz in range(8):
                spot = (sx * 2 + sy) * 8 + sz
                for part in range(2):
                    cube = jnp.zeros((FOOT, LANES), jnp.float32)
                    for second in range(8):
                        moved = rolled(planes[part * 8 + second + 1], FOOT * (second - sz), 1)
                        cube = jnp.where(group == second, moved, cube)
                    records[spot, pl.ds(0, FOOT), part * LANES : (part + 1) * LANES] = cube
                if sz > 0:
                    z_low = rolled(upper, 2 * FOOT - FOOT * (sz - 1), 1)
                else:
                    z_low = rolled(z_in[2, 0, rows, :], 2 * FOOT - FOOT * sy, 1)
                if sz < 7:
                    z_high = rolled(lower, 3 * FOOT - FOOT * (sz + 1), 1)
                else:
                    z_high = rolled(z_in[2, 1, rows, :], 3 * FOOT - FOOT * sy, 1)
                face = jnp.where(group == 0, rolled(planes[0], -FOOT * sz, 1), 0.0)
                face = jnp.where(group == 1, rolled(planes[FOOT + 1], FOOT - FOOT * sz, 1), face)
                face = jnp.where(group == 2, z_low, face)
                face = jnp.where(group == 3, z_high, face)
                records[spot, pl.ds(FOOT, 8), 0:LANES] = face[0:8] + rolled(face[8:16], 64, 1)
                side_rows = jnp.zeros((8, LANES), jnp.float32)
                for number, turned in enumerate(ends):
                    side_rows = jnp.where(row8 == number, turned[sz : sz + 1], side_rows)
                records[spot, pl.ds(FOOT, 8), LANES : 2 * LANES] = side_rows

    records[SPOTS] = jnp.zeros((REC, FOOT * FOOT), jnp.float32)

    def own(owner, slot):
        return records[table_smem[8 + slot, owner]]

    def chip_at(step):
        return lax.rem(chip + step + chips, chips)

    places = [(0, half)]
    for left in range(half - 1, 0, -1):
        places += [(0, left), (1, left)]
    places.append((0, 0))
    number_of = {key: number for number, key in enumerate(places)}
    number_of[1, half] = number_of[0, half]
    number_of[1, 0] = number_of[0, 0]

    def step_of(way, left):
        return left if way == 0 else -left

    pre_copies = []
    for number, (way, left) in enumerate(places):
        target = chip_at(-sign * step_of(way, left)) * 2 + 1 - core
        for slot in range(SLOTS):
            pre_out[number, pl.ds(slot * REC, REC), :] = own(target, slot)
        pre_copies.append(
            send(pre_out.at[number], pre_in.at[number], pre_send.at[number], pre_recv.at[number], {"gz": pair})
        )
    started += pre_copies

    def begins(way, slot):
        return half if slot in takes[way] else half - 1

    arrived = set()
    chain_copies = {}
    for left in range(half, 0, -1):
        for way in range(2):
            number = number_of[way, left]
            target = chip_at(sign * step_of(way, left)) * 2 + core
            for slot in range(SLOTS):
                if left > begins(way, slot):
                    continue
                if number not in arrived:
                    pre_copies[number].wait_recv()
                    arrived.add(number)
                value = own(target, slot) + pre_in[number, pl.ds(slot * REC, REC), :]
                if left < begins(way, slot):
                    chain_copies[way, left, slot].wait_recv()
                    value += chain_in[way, left, slot]
                chain_out[way, left - 1, slot] = value
                chain_copies[way, left - 1, slot] = send(
                    chain_out.at[way, left - 1, slot],
                    chain_in.at[way, left - 1, slot],
                    chain_send.at[way, left - 1, slot],
                    chain_recv.at[way, left - 1, slot],
                    {"gz": ring[way]},
                )
    started += list(chain_copies.values())
    number = number_of[0, 0]
    pre_copies[number].wait_recv()
    for slot in range(SLOTS):
        value = own(me, slot) + pre_in[number, pl.ds(slot * REC, REC), :]
        for way in range(2):
            if begins(way, slot) > 0:
                chain_copies[way, 0, slot].wait_recv()
                value += chain_in[way, 0, slot]
        record_ref[pl.ds(slot * REC, REC), :] = value
    for copy in started:
        copy.wait_send()


def vmem():
    return pl.BlockSpec(memory_space=pltpu.VMEM)


def smem():
    return pl.BlockSpec(memory_space=pltpu.SMEM)


def per_device(sizes, fine_rhs, coarse_rhs, patch_count, patch_corner):
    n_z = sizes[2]
    half = n_z // 4
    f32 = jnp.float32
    fine = fine_rhs.reshape(SLOTS * EDGE, EDGE * EDGE)
    averages, codes = pl.pallas_call(
        pre_kernel,
        out_shape=(
            jax.ShapeDtypeStruct((SLOTS * FOOT, FOOT * FOOT), f32),
            jax.ShapeDtypeStruct((8, LANES), jnp.int32),
        ),
        in_specs=[smem(), smem(), vmem()],
        out_specs=(vmem(), vmem()),
        scratch_shapes=[pltpu.VMEM((2, SLOTS * EDGE, LANES), f32)],
        name="pre",
    )(patch_count, patch_corner, fine)
    rows = EDGE * EDGE
    padded = (EDGE + 2) * EDGE
    record = SLOTS * REC
    dma = pltpu.SemaphoreType.DMA
    coarse_solution, loops = pl.pallas_call(
        functools.partial(coarse_kernel, sizes),
        out_shape=(
            jax.ShapeDtypeStruct((rows, LANES), f32),
            jax.ShapeDtypeStruct((record, FOOT * FOOT), f32),
        ),
        in_specs=[vmem(), vmem(), vmem()],
        out_specs=(vmem(), vmem()),
        scratch_shapes=[
            pltpu.VMEM((n_z * SLOTS, FOOT, FOOT * FOOT), f32),
            pltpu.VMEM((n_z, 8, LANES), jnp.int32),
            pltpu.VMEM((16, LANES), jnp.int32),
            pltpu.SMEM((16, LANES), jnp.int32),
            pltpu.VMEM((padded, LANES), f32),
            pltpu.VMEM((padded, LANES), f32),
            pltpu.VMEM((padded, LANES), f32),
            pltpu.VMEM((3, 2, EDGE, LANES), f32),
            pltpu.VMEM((3, 2, EDGE, LANES), f32),
            pltpu.VMEM((3, 2, EDGE, LANES), f32),
            pltpu.VMEM((3, 2, EDGE, LANES), f32),
            pltpu.VMEM((SPOTS + 1, REC, FOOT * FOOT), f32),
            pltpu.VMEM((2 * half, record, FOOT * FOOT), f32),
            pltpu.VMEM((2 * half, record, FOOT * FOOT), f32),
            pltpu.VMEM((2, half, SLOTS, REC, FOOT * FOOT), f32),
            pltpu.VMEM((2, half, SLOTS, REC, FOOT * FOOT), f32),
            dma((2, half, SLOTS + 1)),
            dma((2, half, SLOTS + 1)),
            dma((2, half + 1, SLOTS + 1)),
            dma((2, half + 1, SLOTS + 1)),
            dma((3, 6)),
            dma((3, 6)),
            dma((2 * half,)),
            dma((2 * half,)),
            dma((2, half, SLOTS)),
            dma((2, half, SLOTS)),
            dma,
        ],
        compiler_params=pltpu.CompilerParams(
            collective_id=0, has_side_effects=True, vmem_limit_bytes=32 * 1024 * 1024
        ),
        name="coarse",
    )(codes, averages, coarse_rhs.reshape(rows, LANES))
    fine_solution = pl.pallas_call(
        post_kernel,
        out_shape=jax.ShapeDtypeStruct(fine.shape, f32),
        in_specs=[smem(), vmem(), vmem()],
        out_specs=vmem(),
        scratch_shapes=[
            pltpu.VMEM((2, SLOTS * EDGE, LANES), f32),
            pltpu.VMEM((SLOTS * EDGE, LANES), f32),
        ],
        name="post",
    )(patch_count, fine, loops)
    return fine_solution.reshape(fine_rhs.shape), coarse_solution.reshape(coarse_rhs.shape)


def solution(mesh):
    sizes = tuple(mesh.shape[axis] for axis in ("gx", "gy", "gz"))
    return jax.shard_map(
        functools.partial(per_device, sizes),
        mesh=mesh,
        in_specs=(
            P(("gx", "gy", "gz"), None, None),
            P("gx", "gy", "gz"),
            P(("gx", "gy", "gz")),
            P(("gx", "gy", "gz"), None),
        ),
        out_specs=(P(("gx", "gy", "gz"), None, None), P("gx", "gy", "gz")),
        check_vma=False,
    )
```
